32 devices in a mesh: chan: 8 (over y, x, core), tm: 4 (over z).
Axes of the slice: x: 2, y: 2, z: 4, core: 2. Of those that a mesh axis runs over, the one named last changes fastest.
Arguments:
- record: bfloat16 [128, 2048], P('chan', 'tm'), may hold values from -6 to 6
- tail: bfloat16 [128, 255], P('chan'), may hold values from -6 to 6
- templates: bfloat16 [128, 128, 128], P(None, 'chan'), may hold values from -6 to 6
- shifts: int32 [128, 128], P(None, 'chan'), may hold values from 0 to 127
- mask: int32 [128], P('chan'), may hold values 0 or 1
Outputs:
- stack: float32 [128, 2048], P('chan', 'tm')
The draws below stay inside these ranges and needn't reach their ends.
All inputs are finite; a program needn't handle non-finite values. No bound on the sum of `mask` on one device may be relied on, other than what follows from the above.
Results may differ from the reference program's by a relative error of at most 0.0029.
Values may be sent and summed in bfloat16 or wider, within the bound.
A program may use at most 64 MiB of HBM per device.

```python
import jax
import jax.numpy as jnp
from jax import lax

NCH = 128
K = 128
L = 128
MS = 128
NS = 2048
H = 255


def with_ends(entries, rng, smallest, largest):
    shape = entries.shape
    place = [jax.random.randint(jax.random.fold_in(rng, axis), (), 0, shape[axis]) for axis in range(len(shape))]
    entries = entries.at[tuple(place)].set(smallest)
    longest = shape.index(max(shape))
    place[longest] = (place[longest] + 1) % shape[longest]
    return entries.at[tuple(place)].set(largest)


def level_of(own_key, shape, cuts, least, high):
    factor_of = 1.0
    for position, parts in cuts:
        steps = jax.random.uniform(jax.random.fold_in(jax.random.fold_in(own_key, 6), position), (parts,), jnp.float32, least / len(cuts), high / len(cuts))
        factor_of = factor_of * jnp.repeat(jnp.exp(steps), shape[position] // parts).reshape((-1,) + (1,) * (len(shape) - 1 - position))
    return factor_of


def centred(stream_key, dims, scale, limit, cuts=(), kind=jnp.bfloat16):
    drawn = scale * jax.random.normal(stream_key, dims, jnp.float32)
    if cuts:
        drawn = drawn * level_of(stream_key, dims, cuts, -0.22, 0.18)
    return jnp.clip(drawn, -limit, limit).astype(kind)


def setup_inputs(seed: int = 0) -> dict:
    key_of = jax.random.split(jax.random.key(seed), 6)
    record = centred(key_of[0], (NCH, NS), 1.0, 6.0, ((0, 8), (1, 4)))
    tail = centred(key_of[1], (NCH, H), 1.0, 6.0, ((0, 8),))
    templates = centred(key_of[2], (K, NCH, L), 1.0, 6.0, ((1, 8),))
    shifts = with_ends(jax.random.randint(key_of[3], (K, NCH), 0, MS), jax.random.fold_in(key_of[3], 1), 0, MS - 1).astype(jnp.int32)
    mask = with_ends((jax.random.randint(key_of[4], (NCH,), 0, 4) < 3).astype(jnp.int32), jax.random.fold_in(key_of[4], 1), 0, 1)
    return {"record": record, "tail": tail, "templates": templates, "shifts": shifts, "mask": mask}


def unit_templates(templates):
    values = templates.astype(jnp.float32)
    tap_count = templates.shape[2]
    centered = values - lax.optimization_barrier(jnp.mean(values, axis=2, keepdims=True))
    norm = jnp.sqrt(tap_count * (lax.optimization_barrier(jnp.mean(centered * centered, axis=2, keepdims=True)) + 1e-06))
    return (centered / norm).astype(jnp.bfloat16)

def window_spread(samples, tap_count):
    values = samples.astype(jnp.float32)
    zero = jnp.zeros((1,), jnp.float32)
    sums = jnp.concatenate([zero, jnp.cumsum(values)])
    squares = jnp.concatenate([zero, jnp.cumsum(values * values)])
    window = sums[tap_count:] - sums[:-tap_count]
    power = squares[tap_count:] - squares[:-tap_count]
    return jnp.sqrt(power - window * window / tap_count + tap_count * 1e-06)

def reference(record, tail, templates, shifts, mask):
    extended = jnp.concatenate([record, tail], axis=1)
    unit = unit_templates(templates).astype(jnp.float32)
    tap_count = templates.shape[2]
    out_len = record.shape[1]
    weights = mask.astype(jnp.float32)
    total = jnp.maximum(jnp.sum(weights), 1.0)

    def pick_lags(series, start):
        return lax.dynamic_slice_in_dim(series, start, out_len)

    def add_channel(running, index):
        samples = lax.dynamic_index_in_dim(extended, index, 0, keepdims=False)
        kernel = lax.dynamic_index_in_dim(unit, index, 1, keepdims=False)
        product = lax.conv_general_dilated(samples.astype(jnp.float32)[None, None, :], kernel[:, None, :], (1,), 'VALID', preferred_element_type=jnp.float32)[0]
        spread = window_spread(samples, tap_count)
        normed = product / spread[None, :]
        offsets = lax.dynamic_index_in_dim(shifts, index, 1, keepdims=False)
        aligned = jax.vmap(pick_lags)(normed, offsets)
        weight = lax.dynamic_index_in_dim(weights, index, 0, keepdims=False)
        return (running + weight * aligned, None)
    start_acc = jnp.zeros((templates.shape[0], out_len), jnp.float32)
    running, _ = lax.scan(add_channel, start_acc, jnp.arange(record.shape[0], dtype=jnp.int32))
    return running * jnp.sqrt(tap_count / total)
```

```python
import functools

import jax
import jax.numpy as jnp
from jax import lax
from jax.experimental import pallas as pl
from jax.experimental.pallas import tpu as pltpu
from jax.sharding import PartitionSpec as P

MESH = pl.DeviceIdType.MESH
LANES = 128
SUBLANES = 8
WIRE = jnp.float32


def ahead(values, distance):
    width = values.shape[1]
    distance = distance % width
    if distance == 0:
        return values
    return pltpu.roll(values, width - distance, 1)


def hankel(samples, tap_count, lag_count):
    width = samples.shape[1]
    rows = jnp.broadcast_to(samples, (SUBLANES, width))
    row = lax.broadcasted_iota(jnp.int32, (SUBLANES, width), 0)
    for bit in range(3):
        rows = jnp.where((row >> bit) & 1 == 1, ahead(rows, 1 << bit), rows)
    groups = [ahead(rows, start)[:, :lag_count] for start in range(0, tap_count, SUBLANES)]
    return jnp.concatenate(groups, axis=0).astype(jnp.bfloat16)


def kernel(n_chan, n_tm, record, tail, templates, shifts, mask, out, ext, halo, inverse, unit, normed,
           part, landed, tally, tallies, send_sem, recv_sem, tally_send, tally_recv, halo_send, halo_recv):
    chan = lax.axis_index("chan")
    tm = lax.axis_index("tm")
    chan_count, out_len = record.shape
    templ_count, _, tap_count = templates.shape
    halo_len = tail.shape[1]
    halo_width = halo.shape[1]
    lag_count = out_len + LANES
    rows = templ_count // n_chan

    barrier = pltpu.get_barrier_semaphore()
    for i in range(1, n_chan):
        pl.semaphore_signal(barrier, inc=1, device_id={"chan": lax.rem(chan + i, n_chan)}, device_id_type=MESH)

    @pl.when(tm > 0)
    def _():
        pl.semaphore_signal(barrier, inc=1, device_id={"tm": tm - 1}, device_id_type=MESH)

    @pl.when(tm < n_tm - 1)
    def _():
        pl.semaphore_signal(barrier, inc=1, device_id={"tm": tm + 1}, device_id_type=MESH)

    count = mask[0]
    for c in range(1, chan_count):
        count = count + mask[c]
    tally[...] = jnp.full(tally.shape, count, jnp.int32).astype(jnp.float32)
    ext[:, :out_len] = record[...].astype(jnp.float32)

    group = min(16, templ_count)

    def normalise(i, carry):
        values = templates[pl.ds(i * group, group)].astype(jnp.float32).reshape(group * chan_count, tap_count)
        centered = values - jnp.sum(values, axis=1, keepdims=True) * (1.0 / tap_count)
        power = jnp.sum(centered * centered, axis=1, keepdims=True) * (1.0 / tap_count)
        scale = 1.0 / jnp.sqrt(tap_count * (power + 1e-06))
        unit[pl.ds(pl.multiple_of(i * group * chan_count, SUBLANES), group * chan_count), :] = centered * scale
        return carry

    lax.fori_loop(0, templ_count // group, normalise, 0)

    neighbours = jnp.minimum(tm, 1) + jnp.minimum(n_tm - 1 - tm, 1)
    pl.semaphore_wait(barrier, n_chan - 1 + neighbours)

    halo_copy = pltpu.make_async_remote_copy(
        src_ref=record.at[:, pl.ds(0, halo_width)], dst_ref=halo, send_sem=halo_send, recv_sem=halo_recv,
        device_id={"tm": jnp.maximum(tm - 1, 0)}, device_id_type=MESH)

    def tally_copy(i):
        return pltpu.make_async_remote_copy(
            src_ref=tally, dst_ref=tallies.at[i], send_sem=tally_send.at[i], recv_sem=tally_recv.at[i],
            device_id={"chan": lax.rem(chan + i, n_chan)}, device_id_type=MESH)

    def part_copy(i):
        return pltpu.make_async_remote_copy(
            src_ref=part.at[i], dst_ref=landed.at[i], send_sem=send_sem.at[i], recv_sem=recv_sem.at[i],
            device_id={"chan": lax.rem(chan + i, n_chan)}, device_id_type=MESH)

    @pl.when(tm > 0)
    def _():
        halo_copy.start()

    for i in range(1, n_chan):
        tally_copy(i).start()

    @pl.when(tm < n_tm - 1)
    def _():
        halo_copy.wait_recv()
        ext[:, out_len:] = halo[...].astype(jnp.float32)

    @pl.when(tm == n_tm - 1)
    def _():
        ext[:, out_len:] = jnp.zeros((chan_count, halo_width), jnp.float32)
        ext[:, out_len:out_len + halo_len] = tail[...].astype(jnp.float32)

    sums = ext[...]
    squares = sums * sums
    for bit in range(tap_count.bit_length() - 1):
        sums = sums + ahead(sums, 1 << bit)
        squares = squares + ahead(squares, 1 << bit)
    window = sums[:, :lag_count]
    variance = jnp.maximum(squares[:, :lag_count] - window * window * (1.0 / tap_count), 0.0)
    inverse[...] = 1.0 / jnp.sqrt(variance + tap_count * 1e-06)

    def correlate(c, carry):
        taps = unit[pl.ds(c, templ_count, stride=chan_count), :].astype(jnp.bfloat16)
        product = jnp.dot(taps, hankel(ext[pl.ds(c, 1), :], tap_count, lag_count),
                          preferred_element_type=jnp.float32)
        weight = jnp.full((1, lag_count), mask[c], jnp.int32).astype(jnp.float32)
        normed[c] = product * (inverse[pl.ds(c, 1), :] * weight)
        return carry

    lax.fori_loop(0, chan_count, correlate, 0, unroll=4)

    def block_sum(block):
        place = pl.ds(pl.multiple_of(block * rows, SUBLANES), rows)
        moveouts = shifts[place, :]
        lane = lax.broadcasted_iota(jnp.int32, (rows, LANES), 1)
        tiles = out_len // LANES
        totals = [jnp.zeros((rows, LANES), jnp.float32)] * tiles
        for c in range(chan_count):
            position = lane + moveouts[:, c:c + 1]
            index = position & (LANES - 1)
            inside = position < LANES
            turned = [
                jnp.take_along_axis(normed[c, place, pl.ds(b * LANES, LANES)], index, axis=1,
                                    mode="promise_in_bounds")
                for b in range(tiles + 1)
            ]
            totals = [totals[b] + jnp.where(inside, turned[b], turned[b + 1]) for b in range(tiles)]
        return jnp.concatenate(totals, axis=1)

    def ship(i, carry):
        part[i] = block_sum(lax.rem(chan + i, n_chan)).astype(part.dtype)
        part_copy(i).start()
        return carry

    lax.fori_loop(1, n_chan, ship, 0)
    total = block_sum(chan)
    number = tally[...]
    for i in range(1, n_chan):
        tally_copy(i).wait_recv()
        number = number + tallies[i]
    scale = jnp.sqrt(tap_count / jnp.maximum(number[0:1, :], 1.0))
    for i in range(1, n_chan):
        part_copy(i).wait_recv()
        total = total + landed[i].astype(jnp.float32)
    for b in range(out_len // LANES):
        span = slice(b * LANES, (b + 1) * LANES)
        out[:, span] = total[:, span] * scale

    for i in range(1, n_chan):
        tally_copy(i).wait_send()
        part_copy(i).wait_send()

    @pl.when(tm > 0)
    def _():
        halo_copy.wait_send()


def shards(n_chan, n_tm, record, tail, templates, shifts, mask):
    chan_count, out_len = record.shape
    templ_count, _, tap_count = templates.shape
    halo_len = tail.shape[1]
    halo_width = -(-halo_len // LANES) * LANES
    lag_count = out_len + LANES
    rows = templ_count // n_chan
    assert tap_count == LANES and halo_len - tap_count < LANES and out_len % LANES == 0
    vmem = pl.BlockSpec(memory_space=pltpu.VMEM)
    f32 = jnp.float32
    dma = pltpu.SemaphoreType.DMA
    return pl.pallas_call(
        functools.partial(kernel, n_chan, n_tm),
        out_shape=jax.ShapeDtypeStruct((rows, out_len), f32),
        in_specs=[vmem, vmem, vmem, vmem, pl.BlockSpec(memory_space=pltpu.SMEM)],
        out_specs=vmem,
        scratch_shapes=[
            pltpu.VMEM((chan_count, out_len + halo_width), f32),
            pltpu.VMEM((chan_count, halo_width), record.dtype),
            pltpu.VMEM((chan_count, lag_count), f32),
            pltpu.VMEM((templ_count * chan_count, tap_count), f32),
            pltpu.VMEM((chan_count, templ_count, lag_count), f32),
            pltpu.VMEM((n_chan, rows, out_len), WIRE),
            pltpu.VMEM((n_chan, rows, out_len), WIRE),
            pltpu.VMEM((SUBLANES, LANES), f32),
            pltpu.VMEM((n_chan, SUBLANES, LANES), f32),
            dma((n_chan,)), dma((n_chan,)), dma((n_chan,)), dma((n_chan,)), dma, dma,
        ],
        compiler_params=pltpu.CompilerParams(collective_id=0, has_side_effects=True),
        name="matched_stack",
    )(record, tail, templates, shifts, mask)


def solution(mesh):
    in_specs = (P("chan", "tm"), P("chan", None), P(None, "chan", None), P(None, "chan"), P("chan"))
    body = functools.partial(shards, mesh.shape["chan"], mesh.shape["tm"])
    return jax.shard_map(body, mesh=mesh, in_specs=in_specs, out_specs=P("chan", "tm"), check_vma=False)
```

```python
import functools

import jax
import jax.numpy as jnp
from jax import lax
from jax.experimental import pallas as pl
from jax.experimental.pallas import tpu as pltpu
from jax.sharding import PartitionSpec as P

MESH = pl.DeviceIdType.MESH
LANES = 128
SUBLANES = 8
WIRE = jnp.float32
NORM_UNROLL = 2
CORR_UNROLL = 8


def ahead(values, distance):
    width = values.shape[1]
    distance = distance % width
    if distance == 0:
        return values
    return pltpu.roll(values, width - distance, 1)


def hankel(samples, tap_count, lag_count):
    width = samples.shape[1]
    rows = jnp.broadcast_to(samples, (SUBLANES, width))
    row = lax.broadcasted_iota(jnp.int32, (SUBLANES, width), 0)
    for bit in range(3):
        rows = jnp.where((row >> bit) & 1 == 1, ahead(rows, 1 << bit), rows)
    groups = [ahead(rows, start)[:, :lag_count] for start in range(0, tap_count, SUBLANES)]
    return jnp.concatenate(groups, axis=0).astype(jnp.bfloat16)


def kernel(n_chan, n_tm, record_in, tail_in, templates_in, shifts_in, mask_in, out, record, tail, templates, shifts,
           mask, ext, halo, inverse, unit, positions, normed, part, landed, tally, tallies,
           load_sem, send_sem, recv_sem, tally_send, tally_recv, halo_send, halo_recv):
    chan = lax.axis_index("chan")
    tm = lax.axis_index("tm")
    chan_count, out_len = record.shape
    templ_count, _, tap_count = templates.shape
    halo_len = tail.shape[1]
    halo_width = halo.shape[1]
    rows = templ_count // n_chan
    early = out_len - LANES
    f32 = jnp.float32

    barrier = pltpu.get_barrier_semaphore()

    @pl.when(tm > 0)
    def _():
        pl.semaphore_signal(barrier, inc=1, device_id={"tm": tm - 1}, device_id_type=MESH)

    @pl.when(tm < n_tm - 1)
    def _():
        pl.semaphore_signal(barrier, inc=1, device_id={"tm": tm + 1}, device_id_type=MESH)

    for i in range(1, n_chan):
        pl.semaphore_signal(barrier, inc=1, device_id={"chan": lax.rem(chan + i, n_chan)}, device_id_type=MESH)

    pairs = ((record_in, record), (shifts_in, shifts), (templates_in, templates), (mask_in, mask), (tail_in, tail))
    record_load, shifts_load, templates_load, mask_load, tail_load = [
        pltpu.make_async_copy(source, place, load_sem.at[i]) for i, (source, place) in enumerate(pairs)]
    for load in (record_load, shifts_load, templates_load, mask_load, tail_load):
        load.start()

    record_load.wait()
    ext[:, :out_len] = record[...].astype(f32)

    shifts_load.wait()
    channel = lax.broadcasted_iota(jnp.int32, (chan_count, chan_count * LANES), 0)
    owner = lax.broadcasted_iota(jnp.int32, (chan_count, chan_count * LANES), 1) // LANES
    spreader = jnp.where(channel == owner, 1.0, 0.0).astype(jnp.bfloat16)
    moveouts = lax.dot_general(shifts[...].astype(f32).astype(jnp.bfloat16), spreader, (((0,), (0,)), ((), ())),
                               preferred_element_type=f32)
    lane = lax.broadcasted_iota(jnp.int32, (templ_count, chan_count * LANES), 1) & (LANES - 1)
    positions[...] = moveouts.astype(jnp.int32) + lane

    mask_load.wait()
    count = mask[0]
    for c in range(1, chan_count):
        count = count + mask[c]
    tally[...] = jnp.full(tally.shape, count, jnp.int32).astype(f32)

    neighbours = jnp.minimum(tm, 1) + jnp.minimum(n_tm - 1 - tm, 1)
    pl.semaphore_wait(barrier, n_chan - 1 + neighbours)

    halo_copy = pltpu.make_async_remote_copy(
        src_ref=record.at[:, pl.ds(0, halo_width)], dst_ref=halo, send_sem=halo_send, recv_sem=halo_recv,
        device_id={"tm": jnp.maximum(tm - 1, 0)}, device_id_type=MESH)

    def tally_copy(i):
        return pltpu.make_async_remote_copy(
            src_ref=tally, dst_ref=tallies.at[i], send_sem=tally_send.at[i], recv_sem=tally_recv.at[i],
            device_id={"chan": lax.rem(chan + i, n_chan)}, device_id_type=MESH)

    def part_copy(i):
        return pltpu.make_async_remote_copy(
            src_ref=part.at[i], dst_ref=landed.at[i], send_sem=send_sem.at[i], recv_sem=recv_sem.at[i],
            device_id={"chan": lax.rem(chan + i, n_chan)}, device_id_type=MESH)

    @pl.when(tm > 0)
    def _():
        halo_copy.start()

    for i in range(1, n_chan):
        tally_copy(i).start()

    templates_load.wait()
    group = min(16, templ_count)

    def normalise(i, carry):
        values = templates[pl.ds(i * group, group)].astype(f32).reshape(group * chan_count, tap_count)
        centered = values - jnp.sum(values, axis=1, keepdims=True) * (1.0 / tap_count)
        power = jnp.sum(centered * centered, axis=1, keepdims=True) * (1.0 / tap_count)
        scale = 1.0 / jnp.sqrt(tap_count * (power + 1e-06))
        unit[pl.ds(pl.multiple_of(i * group * chan_count, SUBLANES), group * chan_count), :] = centered * scale
        return carry

    lax.fori_loop(0, templ_count // group, normalise, 0, unroll=NORM_UNROLL)

    def correlate_span(start, width):
        lags = width - tap_count
        sums = ext[:, start:start + width]
        squares = sums * sums
        for bit in range(tap_count.bit_length() - 1):
            sums = sums + ahead(sums, 1 << bit)
            squares = squares + ahead(squares, 1 << bit)
        window = sums[:, :lags]
        variance = jnp.maximum(squares[:, :lags] - window * window * (1.0 / tap_count), 0.0)
        inverse[:, start:start + lags] = 1.0 / jnp.sqrt(variance + tap_count * 1e-06)

        def correlate(c, carry):
            taps = unit[pl.ds(c, templ_count, stride=chan_count), :].astype(jnp.bfloat16)
            product = jnp.dot(taps, hankel(ext[pl.ds(c, 1), start:start + width], tap_count, lags),
                              preferred_element_type=f32)
            weight = jnp.full((1, lags), mask[c], jnp.int32).astype(f32)
            normed[c, :, start:start + lags] = product * (inverse[pl.ds(c, 1), start:start + lags] * weight)
            return carry

        lax.fori_loop(0, chan_count, correlate, 0, unroll=CORR_UNROLL)

    correlate_span(0, out_len)
    tail_load.wait()

    @pl.when(tm < n_tm - 1)
    def _():
        halo_copy.wait_recv()
        ext[:, out_len:] = halo[...].astype(f32)

    @pl.when(tm == n_tm - 1)
    def _():
        ext[:, out_len:] = jnp.zeros((chan_count, halo_width), f32)
        ext[:, out_len:out_len + halo_len] = tail[...].astype(f32)

    correlate_span(early, LANES + halo_width)

    def block_sum(block):
        place = pl.ds(pl.multiple_of(block * rows, SUBLANES), rows)
        tiles = out_len // LANES
        totals = [jnp.zeros((rows, LANES), f32)] * tiles
        for c in range(chan_count):
            position = positions[place, c * LANES:(c + 1) * LANES]
            index = position & (LANES - 1)
            inside = position < LANES
            turned = [
                jnp.take_along_axis(normed[c, place, pl.ds(b * LANES, LANES)], index, axis=1,
                                    mode="promise_in_bounds")
                for b in range(tiles + 1)
            ]
            totals = [totals[b] + jnp.where(inside, turned[b], turned[b + 1]) for b in range(tiles)]
        return jnp.concatenate(totals, axis=1)

    def ship(i, carry):
        part[i] = block_sum(lax.rem(chan + i, n_chan)).astype(part.dtype)
        part_copy(i).start()
        return carry

    lax.fori_loop(1, n_chan, ship, 0)
    total = block_sum(chan)
    number = tally[...]
    for i in range(1, n_chan):
        tally_copy(i).wait_recv()
        number = number + tallies[i]
    scale = jnp.sqrt(tap_count / jnp.maximum(number[0:1, :], 1.0))
    for i in range(1, n_chan):
        part_copy(i).wait_recv()
        total = total + landed[i].astype(f32)
    for b in range(out_len // LANES):
        span = slice(b * LANES, (b + 1) * LANES)
        out[:, span] = total[:, span] * scale

    for i in range(1, n_chan):
        tally_copy(i).wait_send()
        part_copy(i).wait_send()

    @pl.when(tm > 0)
    def _():
        halo_copy.wait_send()


def shards(n_chan, n_tm, record, tail, templates, shifts, mask):
    chan_count, out_len = record.shape
    templ_count, _, tap_count = templates.shape
    halo_len = tail.shape[1]
    halo_width = -(-halo_len // LANES) * LANES
    lag_count = out_len + LANES
    rows = templ_count // n_chan
    assert tap_count == LANES and halo_len - tap_count < LANES and out_len % LANES == 0 and out_len > LANES
    by_channel = shifts.T
    operands = (record, tail, templates, by_channel, mask)
    f32 = jnp.float32
    dma = pltpu.SemaphoreType.DMA
    return pl.pallas_call(
        functools.partial(kernel, n_chan, n_tm),
        out_shape=pltpu.VMEM((rows, out_len), f32),
        in_specs=[pl.BlockSpec(memory_space=pl.ANY)] * len(operands),
        out_specs=pl.BlockSpec(memory_space=pltpu.VMEM),
        scratch_shapes=[
            pltpu.VMEM(record.shape, record.dtype),
            pltpu.VMEM(tail.shape, tail.dtype),
            pltpu.VMEM(templates.shape, templates.dtype),
            pltpu.VMEM(by_channel.shape, shifts.dtype),
            pltpu.SMEM(mask.shape, mask.dtype),
            pltpu.VMEM((chan_count, out_len + halo_width), f32),
            pltpu.VMEM((chan_count, halo_width), record.dtype),
            pltpu.VMEM((chan_count, lag_count), f32),
            pltpu.VMEM((templ_count * chan_count, tap_count), f32),
            pltpu.VMEM((templ_count, chan_count * LANES), jnp.int32),
            pltpu.VMEM((chan_count, templ_count, lag_count), f32),
            pltpu.VMEM((n_chan, rows, out_len), WIRE),
            pltpu.VMEM((n_chan, rows, out_len), WIRE),
            pltpu.VMEM((SUBLANES, LANES), f32),
            pltpu.VMEM((n_chan, SUBLANES, LANES), f32),
            dma((len(operands),)), dma((n_chan,)), dma((n_chan,)), dma((n_chan,)), dma((n_chan,)), dma, dma,
        ],
        compiler_params=pltpu.CompilerParams(collective_id=0, has_side_effects=True),
        name="matched_stack",
    )(*operands)


def solution(mesh):
    in_specs = (P("chan", "tm"), P("chan", None), P(None, "chan", None), P(None, "chan"), P("chan"))
    body = functools.partial(shards, mesh.shape["chan"], mesh.shape["tm"])
    return jax.shard_map(body, mesh=mesh, in_specs=in_specs, out_specs=P("chan", "tm"), check_vma=False)
```
